32 devices in a mesh: row: 8 (over z, x), col: 4 (over y, core).
Axes of the slice: x: 2, y: 2, z: 4, core: 2. Of those that a mesh axis runs over, the one named last changes fastest.
Arguments:
- pole_values: float32 [65536], P('row'), may hold values from -32768 to 32768, as said below
- weights: float32 [65536], P('row'), may hold values from 0.15 to 0.5
- centers: float32 [65536], P('col'), as said below
- offsets: float32 [65536], P('col'), may hold values from -0.1 to 0.1
- chosen: int32 [2048], replicated, may hold values from 0 to 65535
- column_pole: int32 [2, 32768], P(None, 'row'), may hold values from 0 to 65535, as said below
- eigen_blocks: bfloat16 [3072, 2, 32768], P('col', None, 'row'), may hold values from -6 to 6
Outputs:
- roots_offset: float32 [65536], P('col')
- panel: float32 [3072, 2, 2048], P(('col', 'row'))
The draws below stay inside these ranges and needn't reach their ends.
Inputs may be any that keep to these rules, and one draw needn't show every extreme that they name: `pole_values`: ascending; consecutive poles differ by 1/4 to 7/4; every pole is a multiple of 1/128. centers[i] is the midpoint of pole_values[i] and pole_values[i + 1]; the last one is the last pole plus 1/2. `chosen`: indices of roots. `column_pole`: each of 0 to 65535 stands once.
All inputs are finite; a program needn't handle non-finite values.
Results may differ from the reference program's by a relative error of at most 0.0021.
Values may be sent and summed in bfloat16 or wider, within the bound.
A program may use at most 128 MiB of HBM per device.

```python
import math
import jax
import jax.numpy as jnp
from jax import lax

N = 65536
H = 32768
ITERS = 3
K = 2048
QROWS = 3072


def pole_layout(key):
    marks = jax.random.randint(jax.random.fold_in(key, 11), (N,), 16, 113)
    return (jnp.arange(N) - N // 2).astype(jnp.float32) + marks.astype(jnp.float32) / 128.0


def draw_pole_values(key, part):
    return pole_layout(key)


def draw_centers(key, part):
    values = pole_layout(key)
    return jnp.concatenate([0.5 * (values[:-1] + values[1:]), values[-1:] + 0.5])


def draw_column_pole(key, part):
    return jax.random.permutation(jax.random.fold_in(key, 5), N).astype(jnp.int32).reshape(2, H)


def plant(drawn, stream_key, smallest, high):
    shape = drawn.shape
    place = [jax.random.randint(jax.random.fold_in(stream_key, axis), (), 0, shape[axis]) for axis in range(len(shape))]
    drawn = drawn.at[tuple(place)].set(smallest)
    longest = shape.index(max(shape))
    place[longest] = (place[longest] + 1) % shape[longest]
    return drawn.at[tuple(place)].set(high)


def steps_of(own_key, shape, shards, smallest, top_value):
    factor_of = 1.0
    for dim, shards_of in shards:
        heights = jax.random.uniform(jax.random.fold_in(jax.random.fold_in(own_key, 6), dim), (shards_of,), jnp.float32, smallest / len(shards), top_value / len(shards))
        factor_of = factor_of * jnp.repeat(jnp.exp(heights), shape[dim] // shards_of).reshape((-1,) + (1,) * (len(shape) - 1 - dim))
    return factor_of


def gaussian(key, dims, scale, most, split=(), dtype=jnp.bfloat16):
    entries = jax.random.normal(key, dims, jnp.float32) * scale
    if len(split) > 0:
        entries = steps_of(key, dims, split, -0.22, 0.18) * entries
    return jnp.clip(entries, min=-most, max=most).astype(dtype)


def setup_inputs(seed: int = 0) -> dict:
    key_of = jax.random.split(jax.random.key(seed), 8)
    pole_values = draw_pole_values(jax.random.fold_in(key_of[7], 71), 0)
    weights = jnp.clip(jnp.exp(math.log(0.5) - 1.2039728 * jax.random.uniform(key_of[1], (N,), jnp.float32) ** steps_of(key_of[1], (N,), ((0, 8),), -0.2, 0.2)), 0.15, 0.5)
    centers = draw_centers(jax.random.fold_in(key_of[7], 71), 0)
    offsets = jnp.clip(jax.random.uniform(key_of[3], (N,), jnp.float32, -0.1, 0.1) * steps_of(key_of[3], (N,), ((0, 4),), -0.4, 0.0), -0.1, 0.1)
    chosen = plant(jax.random.randint(key_of[4], (K,), 0, N), jax.random.fold_in(key_of[4], 1), 0, N - 1).astype(jnp.int32)
    column_pole = draw_column_pole(jax.random.fold_in(key_of[7], 71), 0)
    eigen_blocks = gaussian(key_of[6], (QROWS, 2, H), 1.0, 6.0, ((0, 4), (2, 8)))
    return {"pole_values": pole_values, "weights": weights, "centers": centers, "offsets": offsets, "chosen": chosen, "column_pole": column_pole, "eigen_blocks": eigen_blocks}


def block_sums(pole_vals, weight_sq, center_vals, offset_vals, block_rows):
    root_count = center_vals.shape[0]
    block_rows = min(block_rows, root_count)
    center_blocks = center_vals.reshape(root_count // block_rows, block_rows)
    offset_blocks = offset_vals.reshape(root_count // block_rows, block_rows)

    def per_block(blocks):
        distance = pole_vals[None, :] - blocks[0][:, None] - blocks[1][:, None]
        inverse = 1.0 / distance
        weighted = weight_sq[None, :] * inverse
        return (lax.optimization_barrier(jnp.sum(weighted, axis=1)), lax.optimization_barrier(jnp.sum(weighted * inverse, axis=1)), lax.optimization_barrier(jnp.min(jnp.abs(distance), axis=1)))
    sums = lax.map(per_block, (center_blocks, offset_blocks))
    return tuple((item.reshape(root_count) for item in sums))

def newton_update(offset_now, sum_inverse, sum_square, nearest):
    limit = 0.5 * nearest
    return offset_now - jnp.clip((1.0 + sum_inverse) / sum_square, -limit, limit)

def cauchy_block(pole_picked, weight_picked, panel_center, panel_offset, inv_norm):
    distance = pole_picked[:, None] - panel_center[None, :] - panel_offset[None, :]
    return (weight_picked[:, None] * (1.0 / distance) * inv_norm[None, :]).astype(jnp.bfloat16)

def reference(pole_values, weights, centers, offsets, chosen, column_pole, eigen_blocks):
    weight_sq = weights * weights
    offset_now = offsets
    for iteration in range(ITERS):
        sum_inverse, sum_square, nearest = block_sums(pole_values, weight_sq, centers, offset_now, 128)
        offset_now = newton_update(offset_now, sum_inverse, sum_square, nearest)
    panel_center = centers[chosen]
    panel_offset = offset_now[chosen]
    norm_sq = block_sums(pole_values, weight_sq, panel_center, panel_offset, 64)[1]
    inv_norm = lax.rsqrt(norm_sq)
    halves_out = []
    for half_index in range(2):
        pole_index = column_pole[half_index]
        cauchy = cauchy_block(pole_values[pole_index], weights[pole_index], panel_center, panel_offset, inv_norm)
        halves_out.append(jnp.dot(eigen_blocks[:, half_index, :], cauchy, preferred_element_type=jnp.float32))
    return (offset_now, jnp.stack(halves_out, axis=1))
```

```python
import jax
import jax.numpy as jnp
from jax import lax
from jax.experimental import pallas as pl
from jax.experimental.pallas import tpu as pltpu
from jax.sharding import PartitionSpec as P

ITERS = 3
LANES = 128
GROUP = 4


def pole_sweep(bases_ref, poles_ref, weight_sq_ref, center, offset, square_only):
    tiles = center.shape[0]

    def block(index, sums):
        base = bases_ref[index]
        relative = poles_ref[pl.ds(index, 1), :] - base
        pole_t = jnp.broadcast_to(relative, (LANES, LANES)).T
        weight_t = jnp.broadcast_to(weight_sq_ref[pl.ds(index, 1), :], (LANES, LANES)).T
        root = (center - base) + offset
        inverse_sums, square_sums = list(sums[0]), list(sums[1])
        for first in range(0, tiles, GROUP):
            members = range(first, min(first + GROUP, tiles))
            points = {m: jnp.broadcast_to(root[m : m + 1, :], (8, LANES)) for m in members}
            part_inverse = {m: None for m in members}
            part_square = {m: None for m in members}
            for k in range(LANES // 8):
                pole = pole_t[8 * k : 8 * k + 8, :]
                weight = weight_t[8 * k : 8 * k + 8, :]
                for m in members:
                    inverse = 1.0 / (pole - points[m])
                    weighted = weight * inverse
                    square = weighted * inverse
                    if k == 0:
                        part_inverse[m], part_square[m] = weighted, square
                    else:
                        part_inverse[m] = part_inverse[m] + weighted
                        part_square[m] = part_square[m] + square
            for m in members:
                inverse_sums[m] = inverse_sums[m] + part_inverse[m]
                square_sums[m] = square_sums[m] + part_square[m]
        if square_only:
            inverse_sums = list(sums[0])
        return tuple(inverse_sums), tuple(square_sums)

    zero = tuple(jnp.zeros((8, LANES), jnp.float32) for _ in range(tiles))
    inverse_sums, square_sums = lax.fori_loop(0, poles_ref.shape[0], block, (zero, zero))
    fold = lambda parts: jnp.concatenate([jnp.sum(p, axis=0, keepdims=True) for p in parts], axis=0)
    return None if square_only else fold(inverse_sums), fold(square_sums)


def roots_kernel(bases_ref, poles_ref, weight_sq_ref, center_ref, offset_ref, left_ref, right_ref, out_ref):
    center = center_ref[...]
    to_left = left_ref[...] - center
    to_right = right_ref[...] - center

    def step(_, offset):
        sum_inverse, sum_square = pole_sweep(bases_ref, poles_ref, weight_sq_ref, center, offset, False)
        limit = 0.5 * jnp.minimum(jnp.abs(to_left - offset), jnp.abs(to_right - offset))
        change = (1.0 + sum_inverse) / sum_square
        return offset - jnp.minimum(jnp.maximum(change, -limit), limit)

    out_ref[...] = lax.fori_loop(0, ITERS, step, offset_ref[...])


def norm_kernel(bases_ref, poles_ref, weight_sq_ref, center_ref, offset_ref, out_ref):
    out_ref[...] = pole_sweep(
        bases_ref, poles_ref, weight_sq_ref, center_ref[...], offset_ref[...], True
    )[1]


def run_kernel(kernel, bases, *operands):
    vmem = pl.BlockSpec(memory_space=pltpu.VMEM)
    return pl.pallas_call(
        kernel,
        out_shape=jax.ShapeDtypeStruct(operands[2].shape, jnp.float32),
        in_specs=[pl.BlockSpec(memory_space=pltpu.SMEM)] + [vmem] * len(operands),
        out_specs=vmem,
    )(bases, *operands)


def lookup(tables, index):
    rows = jnp.concatenate([t.reshape(-1, LANES) for t in tables], axis=1)
    high = lax.reduce_precision(rows, 8, 7)
    middle = lax.reduce_precision(rows - high, 8, 7)
    low = (rows - high) - middle
    pieces = jnp.concatenate([high, middle, low], axis=1).astype(jnp.bfloat16)
    pick = (index[:, None] // LANES == jnp.arange(rows.shape[0])[None, :]).astype(jnp.bfloat16)
    found = jnp.dot(pick, pieces, preferred_element_type=jnp.float32)
    width = rows.shape[1]
    found = (found[:, :width] + found[:, width : 2 * width]) + found[:, 2 * width :]
    lane = index[:, None] % LANES == jnp.arange(LANES)[None, :]
    return [
        jnp.sum(jnp.where(lane, found[:, t * LANES : (t + 1) * LANES], 0.0), axis=1)
        for t in range(len(tables))
    ]


def on_device(pole_values, weights, centers, offsets, chosen, column_pole, eigen_blocks):
    gathered = lax.all_gather(jnp.stack([pole_values, weights]), "row", axis=1, tiled=True)
    all_poles, all_weights = gathered[0], gathered[1]
    rows = lax.axis_size("row")
    per_device = offsets.shape[0] // rows
    first_root = lax.axis_index("row") * per_device
    my_first = lax.axis_index("col") * offsets.shape[0] + first_root
    my_centers = lax.dynamic_slice_in_dim(centers, first_root, per_device)
    my_offsets = lax.dynamic_slice_in_dim(offsets, first_root, per_device)
    shifted = jnp.concatenate([all_poles[1:], all_poles[-1:]])
    left = lax.dynamic_slice_in_dim(all_poles, my_first, per_device)
    right = lax.dynamic_slice_in_dim(shifted, my_first, per_device)

    flat = lambda values: values.reshape(-1, LANES)
    pole_rows = flat(all_poles)
    my_offsets = run_kernel(
        roots_kernel,
        pole_rows[:, LANES // 2],
        pole_rows,
        flat(all_weights * all_weights),
        flat(my_centers),
        flat(my_offsets),
        flat(left),
        flat(right),
    ).reshape(-1)

    match = (chosen[:, None] - my_first) == jnp.arange(per_device)[None, :]
    picked = jnp.stack(
        [
            jnp.sum(jnp.where(match, my_centers[None, :], 0.0), axis=1),
            jnp.sum(jnp.where(match, my_offsets[None, :], 0.0), axis=1),
        ]
    )
    panel_center, panel_offset = lax.psum(picked, ("row", "col"))
    offset_now = lax.all_gather(my_offsets, "row", axis=0, tiled=True)
    local_rows = flat(pole_values)
    partial_sq = run_kernel(
        norm_kernel,
        local_rows[:, LANES // 2],
        local_rows,
        flat(weights * weights),
        flat(panel_center),
        flat(panel_offset),
    ).reshape(-1)
    inv_norm = lax.rsqrt(lax.psum(partial_sq, "row"))

    pole_picked, weight_picked = lookup([all_poles, all_weights], column_pole.reshape(-1))
    pole_picked = pole_picked.reshape(column_pole.shape)
    weight_picked = weight_picked.reshape(column_pole.shape)
    halves = []
    for half in range(column_pole.shape[0]):
        distance = (pole_picked[half][:, None] - panel_center[None, :]) - panel_offset[None, :]
        cauchy = (weight_picked[half][:, None] * (1.0 / distance) * inv_norm[None, :]).astype(jnp.bfloat16)
        part = jnp.dot(eigen_blocks[:, half, :], cauchy, preferred_element_type=jnp.float32)
        sent = part.astype(jnp.bfloat16).reshape(rows, -1, part.shape[1])
        got = lax.all_to_all(sent, "row", split_axis=0, concat_axis=0, tiled=True)
        halves.append(jnp.sum(got.astype(jnp.float32), axis=0))
    return (offset_now, jnp.stack(halves, axis=1))


def solution(mesh):
    placed = (P("row"), P("row"), P("col"), P("col"), P(), P(None, "row"), P("col", None, "row"))
    return jax.shard_map(
        on_device,
        mesh=mesh,
        in_specs=placed,
        out_specs=(P("col"), P(("col", "row"), None, None)),
        check_vma=False,
    )
```
